32 devices in a mesh: rep: 1 (over z), dp: 32 (over x, y, core).
Axes of the slice: x: 4, y: 4, z: 1, core: 2. Of those that a mesh axis runs over, the one named last changes fastest.
The devices are a block of a 4x4x8 slice.
Arguments:
- x: bfloat16 [32, 2048, 896], P(('rep', 'dp'))
- dy: bfloat16 [32, 2048, 896], P(('rep', 'dp'))
- w_gate: bfloat16 [2, 896, 2560], replicated
- w_up: bfloat16 [2, 896, 2560], replicated
- w_down: bfloat16 [2, 2560, 896], replicated
- m_w_gate: float32 [2, 896, 2560], replicated
- m_w_up: float32 [2, 896, 2560], replicated
- m_w_down: float32 [2, 2560, 896], replicated
- v_w_gate: float32 [2, 896, 2560], replicated
- v_w_up: float32 [2, 896, 2560], replicated
- v_w_down: float32 [2, 2560, 896], replicated
Outputs:
- output 1: bfloat16 [2, 896, 2560], P('rep')
- output 2: bfloat16 [2, 896, 2560], P('rep')
- output 3: bfloat16 [2, 2560, 896], P('rep')
- output 4: float32 [2, 896, 2560], P('rep')
- output 5: float32 [2, 896, 2560], P('rep')
- output 6: float32 [2, 2560, 896], P('rep')
- output 7: float32 [2, 896, 2560], P('rep')
- output 8: float32 [2, 896, 2560], P('rep')
- output 9: float32 [2, 2560, 896], P('rep')
All inputs are finite; a program needn't handle non-finite values.
Results may differ from the reference program's by a relative error of at most 0.022.
Values are sent between devices in bfloat16 or wider.
A program may use at most 768 MiB of HBM per device.

```python
import jax
import jax.numpy as jnp
from jax import lax

SEQUENCES = 32
TOKENS = 2048
D = 896
FF = 2560
LAYERS = 2
NAMES = ("w_gate", "w_up", "w_down")
SHAPES = {"w_gate": (LAYERS, D, FF), "w_up": (LAYERS, D, FF), "w_down": (LAYERS, FF, D)}


def bump(key, n, height):
    away = (jnp.arange(n, dtype=jnp.int32) - jax.random.randint(key, (), 0, n, jnp.int32)) % n
    return jnp.where(away < n // 8, height, 1.0)


def together(key, own, strength):
    shared = jax.random.normal(key, own.shape[1:], jnp.float32)
    return (own + strength * shared) * lax.rsqrt(1 + strength * strength)


def setup_inputs(seed: int = 0, part: int = 0) -> dict:
    kx, kdy, ka, kb, kz, kf, kh, kl, *keys = jax.random.split(jax.random.key(seed), 8 + 3 * len(NAMES))
    kx, kdy, ka, kb = (jax.random.fold_in(k, part) for k in (kx, kdy, ka, kb))
    kw, km, kv = (keys[i::3] for i in range(3))
    shape = (SEQUENCES, TOKENS, D)
    much_x, much_dy = jax.random.uniform(kz, (2,), jnp.float32, 0.0, 1.0)
    loud = 2.0 ** jax.random.uniform(jax.random.fold_in(kz, 1), (), jnp.float32, -1.0, 2.0)
    layers = 2.0 ** jax.random.uniform(kl, (LAYERS, 1, 1), jnp.float32, -1.0, 1.0)
    x = together(ka, jax.random.normal(kx, shape, jnp.float32), much_x) * bump(kf, D, 4.0)
    dy = together(kb, jax.random.normal(kdy, shape, jnp.float32), much_dy)
    drawn = {"x": x.astype(jnp.bfloat16), "dy": (loud * dy * (SEQUENCES * TOKENS) ** -0.5).astype(jnp.bfloat16)}
    for key, name in zip(kw, NAMES, strict=True):
        w = jax.random.normal(key, SHAPES[name], jnp.float32) * SHAPES[name][1] ** -0.5
        drawn[name] = (w * {"w_gate": 1.0, "w_up": bump(kh, FF, 4.0), "w_down": layers}[name]).astype(jnp.bfloat16)
    for key, name in zip(km, NAMES, strict=True):
        drawn[f"m_{name}"] = 0.1 * jax.random.normal(key, SHAPES[name], jnp.float32)
    for key, name in zip(kv, NAMES, strict=True):
        drawn[f"v_{name}"] = jax.random.uniform(key, SHAPES[name], jnp.float32, 0.005, 0.015)
    return drawn


def matmul(a, w):
    return jnp.dot(a, w, preferred_element_type=jnp.float32).astype(jnp.bfloat16)


def normed(h):
    wide = h.astype(jnp.float32)
    scale = lax.rsqrt(jnp.mean(wide**2, -1, keepdims=True) + 1e-6)
    return (wide * scale).astype(jnp.bfloat16)


def layer(h, w):
    a = normed(h)
    gate = jnp.dot(a, w["w_gate"], preferred_element_type=jnp.float32)
    up = jnp.dot(a, w["w_up"], preferred_element_type=jnp.float32)
    return h + matmul((jax.nn.silu(gate) * up).astype(jnp.bfloat16), w["w_down"])


def adamw(w, m, v, g):
    m = 0.9 * m + 0.1 * g
    v = 0.95 * v + 0.05 * g * g
    step = m * lax.rsqrt(v + 1e-8) + 0.1 * w
    return (w - 0.02 * step).astype(jnp.bfloat16), m, v


def clipped(gradients, sum_of_squares, count):
    factor = jnp.minimum(1.0, 0.5 * lax.rsqrt(sum_of_squares / count + 1e-30))
    return [g * factor for g in gradients]


def stack(weights, h):
    return lax.scan(lambda h, w: (layer(h, w), None), h, weights)[0]


def reference(x, dy, w_gate, w_up, w_down, m_w_gate, m_w_up, m_w_down, v_w_gate, v_w_up, v_w_down):
    weights = dict(zip(NAMES, (w_gate, w_up, w_down), strict=True))

    def take(so_far, sequence):
        h, by_y = sequence
        _, back = jax.vjp(lambda w: stack(w, h), weights)
        return jax.tree.map(lambda total, term: total + term.astype(jnp.float32), so_far, back(by_y)[0]), None

    none_yet = {name: jnp.zeros(w.shape, jnp.float32) for name, w in weights.items()}
    by_weights, _ = lax.scan(take, none_yet, (x, dy))
    gradients = [by_weights[name].astype(jnp.bfloat16).astype(jnp.float32) for name in NAMES]
    gradients = clipped(gradients, sum(jnp.sum(g * g) for g in gradients), sum(g.size for g in gradients))
    new = [
        adamw(w.astype(jnp.float32), m, v, g)
        for w, m, v, g in zip((w_gate, w_up, w_down), (m_w_gate, m_w_up, m_w_down), (v_w_gate, v_w_up, v_w_down), gradients, strict=True)
    ]
    return tuple(one[which] for which in range(3) for one in new)
```

```python
import functools
import math

import jax
import jax.numpy as jnp
from jax import lax
from jax.experimental import pallas as pl
from jax.experimental.pallas import tpu as pltpu
from jax.sharding import PartitionSpec as P

BF, F32 = jnp.bfloat16, jnp.float32
FB = 256
TB = 512
VMEM = 62 * 2**20
NT = (((1,), (1,)), ((), ()))
DONE = pl.BlockSpec((8, 128), lambda *_: (0, 0))


def dot(a, b):
    return jnp.dot(a, b, preferred_element_type=F32)


def dot_nt(a, b):
    return lax.dot_general(a, b, NT, preferred_element_type=F32)


def norm_scale(wide):
    return lax.rsqrt(jnp.mean(wide * wide, -1, keepdims=True) + 1e-6)


def cost(flops, moved):
    return pl.CostEstimate(flops=int(flops), bytes_accessed=int(moved), transcendentals=0)


def params(vmem=VMEM):
    return pltpu.CompilerParams(vmem_limit_bytes=vmem, dimension_semantics=("arbitrary",))


def once(shape, index):
    return pl.BlockSpec(shape, index, pipeline_mode=pl.Buffered(1))


def forward_kernel(h_ref, dy_ref, wg_ref, wu_ref, wd_ref, h1_ref, a1_ref, a1t_ref, a0t_ref, dyt_ref, gate_ref, up_ref, hid):
    ff = wg_ref.shape[2]
    h = h_ref[...]
    wide = h.astype(F32)
    a = (wide * norm_scale(wide)).astype(BF)
    a0t_ref[...] = a.T
    dyt_ref[...] = dy_ref[...].T
    for j in range(0, ff, FB):
        gate = dot(a, wg_ref[0, :, j : j + FB])
        up = dot(a, wu_ref[0, :, j : j + FB])
        gate_ref[:, j : j + FB] = gate
        up_ref[:, j : j + FB] = up
        hid[:, j : j + FB] = (gate * lax.logistic(gate) * up).astype(BF)
    out = dot(hid[...], wd_ref[0]).astype(BF)
    h1 = (h.astype(F32) + out.astype(F32)).astype(BF)
    h1_ref[...] = h1
    wide = h1.astype(F32)
    a1 = (wide * norm_scale(wide)).astype(BF)
    a1_ref[...] = a1
    a1t_ref[...] = a1.T


def forward(layer, h, dy, wg, wu, wd):
    t, d = h.shape
    ff = wg.shape[2]
    rows = pl.BlockSpec((TB, d), lambda i: (i, 0))
    cols = pl.BlockSpec((d, TB), lambda i: (0, i))
    wide = pl.BlockSpec((TB, ff), lambda i: (i, 0))
    whole = [once((1,) + w.shape[1:], lambda i: (layer, 0, 0)) for w in (wg, wu, wd)]
    act, actt = jax.ShapeDtypeStruct((t, d), BF), jax.ShapeDtypeStruct((d, t), BF)
    kept = jax.ShapeDtypeStruct((t, ff), F32)
    return pl.pallas_call(
        forward_kernel,
        grid=(t // TB,),
        in_specs=[rows, rows] + whole,
        out_specs=[rows, rows, cols, cols, cols, wide, wide],
        out_shape=[act, act, actt, actt, actt, kept, kept],
        scratch_shapes=[pltpu.VMEM((TB, ff), BF)],
        compiler_params=params(),
        cost_estimate=cost(6 * t * d * ff, 8 * t * ff),
        name="forward",
    )(h, dy, wg, wu, wd)


def spread(pos_ref, side, scr, g_ref):
    rows = scr.shape[0] // side**2
    for r0 in range(side):
        for r1 in range(side):
            at = lax.rem(pos_ref[1] + r0, side) * side + lax.rem(pos_ref[2] + r1, side)
            g_ref[r0 * side + r1, 0] = scr[pl.ds(pl.multiple_of(at * rows, 8), rows), :].astype(BF)


def backward_of_hidden(gate, up, dh):
    s = lax.logistic(gate)
    silu = gate * s
    by_silu = dh * up
    return (silu * up).astype(BF), (by_silu * (s + silu * (1.0 - s))).astype(BF), (dh * silu).astype(BF)


def weight_gradients(scr, at_ref, dyt_ref, hid, dg_ref, du_ref):
    scr[:, :FB] = dot(at_ref[...], dg_ref[...])
    scr[:, FB : 2 * FB] = dot(at_ref[...], du_ref[...])
    scr[:, 2 * FB :] = dot(dyt_ref[...], hid[...])


def last_kernel(side, pos_ref, a_ref, at_ref, dy_ref, dyt_ref, wg_ref, wu_ref, wd_ref, *rest):
    g_ref, dg_ref, du_ref, hid, scr = rest[-5:]
    for c in range(0, a_ref.shape[0], TB):
        here = slice(c, c + TB)
        gate = dot(a_ref[here, :], wg_ref[0])
        up = dot(a_ref[here, :], wu_ref[0])
        dh = dot_nt(dy_ref[here, :], wd_ref[0]).astype(BF).astype(F32)
        hid[here, :], dg_ref[here, :], du_ref[here, :] = backward_of_hidden(gate, up, dh)
    weight_gradients(scr, at_ref, dyt_ref, hid, dg_ref, du_ref)
    spread(pos_ref, side, scr, g_ref)


def inner_kernel(side, pos_ref, gate_ref, up_ref, at_ref, dy_ref, dyt_ref, wd_ref, *rest):
    g_ref, done_ref, hid, dg, du, scr = rest[-6:]
    done_ref[...] = jnp.zeros_like(done_ref)
    for c in range(0, dy_ref.shape[0], TB):
        here = slice(c, c + TB)
        dh = dot_nt(dy_ref[here, :], wd_ref[0]).astype(BF).astype(F32)
        hid[here, :], dg[here, :], du[here, :] = backward_of_hidden(gate_ref[here, :], up_ref[here, :], dh)
    weight_gradients(scr, at_ref, dyt_ref, hid, dg, du)
    spread(pos_ref, side, scr, g_ref)


def piece_shape(side, d, ff):
    return (side**2, ff // (2 * FB), d // side**2, 3 * FB)


def last_half(side, layer, pos, a, at, dy, dyt, wg, wu, wd, sofar):
    t, d = a.shape
    ff = wg.shape[2]
    nb = ff // (2 * FB)
    whole = [once((t, d), lambda j, p: (0, 0)), once((d, t), lambda j, p: (0, 0))] * 2
    up_block = pl.BlockSpec((1, d, FB), lambda j, p: (layer, 0, p[0] * nb + j))
    down_block = pl.BlockSpec((1, FB, d), lambda j, p: (layer, p[0] * nb + j, 0))
    by_gate = pl.BlockSpec((t, FB), lambda j, p: (0, p[0] * nb + j))
    shape = piece_shape(side, d, ff)
    g_block = pl.BlockSpec((shape[0], 1) + shape[2:], lambda j, p: (0, j, 0, 0))
    kept = jax.ShapeDtypeStruct((t, ff), BF)
    more = [] if sofar is None else list(sofar)
    return pl.pallas_call(
        functools.partial(last_kernel, side),
        grid_spec=pltpu.PrefetchScalarGridSpec(
            num_scalar_prefetch=1,
            grid=(nb,),
            in_specs=whole + [up_block, up_block, down_block] + [pl.BlockSpec(memory_space=pl.ANY)] * len(more),
            out_specs=[g_block, by_gate, by_gate],
            scratch_shapes=[pltpu.VMEM((t, FB), BF), pltpu.VMEM((d, 3 * FB), F32)],
        ),
        out_shape=[jax.ShapeDtypeStruct(shape, BF), kept, kept],
        input_output_aliases={8 + i: 1 + i for i in range(len(more))},
        compiler_params=params(),
        cost_estimate=cost(6 * t * d * ff, 2 * t * ff),
        name="last_half",
    )(pos, a, at, dy, dyt, wg, wu, wd, *more)


def inner_half(side, layer, first, last, pos, gate, up, at, dy, dyt, wd, sofar):
    t, d = dy.shape
    ff = wd.shape[1]
    nb = ff // (2 * FB)
    kept = pl.BlockSpec((t, FB), lambda j, p: (0, p[0] * nb + first + j))
    rows, cols = once((t, d), lambda j, p: (0, 0)), once((d, t), lambda j, p: (0, 0))
    down_block = pl.BlockSpec((1, FB, d), lambda j, p: (layer, p[0] * nb + first + j, 0))
    shape = piece_shape(side, d, ff)
    more = [] if sofar is None else [sofar]
    share = (last - first) / nb
    return pl.pallas_call(
        functools.partial(inner_kernel, side),
        grid_spec=pltpu.PrefetchScalarGridSpec(
            num_scalar_prefetch=1,
            grid=(last - first,),
            in_specs=[kept, kept, cols, rows, cols, down_block] + [pl.BlockSpec(memory_space=pl.ANY)] * len(more),
            out_specs=[pl.BlockSpec((shape[0], 1) + shape[2:], lambda j, p: (0, first + j, 0, 0)), DONE],
            scratch_shapes=[pltpu.VMEM((t, FB), BF)] * 3 + [pltpu.VMEM((d, 3 * FB), F32)],
        ),
        out_shape=[jax.ShapeDtypeStruct(shape, BF), jax.ShapeDtypeStruct((8, 128), F32)],
        input_output_aliases={7 + i: i for i in range(len(more))},
        compiler_params=params(),
        cost_estimate=cost(4 * t * d * ff * share, 4 * t * ff * share),
        name="inner_half",
    )(pos, gate, up, at, dy, dyt, wd, *more)


def input_kernel(dg_ref, du_ref, wg_ref, wu_ref, h_ref, dy_ref, *rest):
    dh_ref, dht_ref, done_ref = rest[-3:]
    done_ref[...] = jnp.zeros_like(done_ref)
    da = dot_nt(dg_ref[...], wg_ref[0]).astype(BF).astype(F32) + dot_nt(du_ref[...], wu_ref[0]).astype(BF).astype(F32)
    da = da.astype(BF).astype(F32)
    wide = h_ref[...].astype(F32)
    s = norm_scale(wide)
    by_wide = da * s - wide * (s * s * s * jnp.mean(da * wide, -1, keepdims=True))
    dh = (dy_ref[...].astype(F32) + by_wide.astype(BF).astype(F32)).astype(BF)
    dh_ref[...] = dh
    dht_ref[...] = dh.T


def input_gradient(layer, part, parts, dg, du, wg, wu, h, dy, sofar):
    t, d = h.shape
    ff = wg.shape[2]
    steps = t // TB // parts
    rows = pl.BlockSpec((TB, d), lambda i: (part * steps + i, 0))
    wide = pl.BlockSpec((TB, ff), lambda i: (part * steps + i, 0))
    whole = once((1, d, ff), lambda i: (layer, 0, 0))
    more = [] if sofar is None else list(sofar)
    return pl.pallas_call(
        input_kernel,
        grid=(steps,),
        in_specs=[wide, wide, whole, whole, rows, rows] + [pl.BlockSpec(memory_space=pl.ANY)] * len(more),
        out_specs=[rows, pl.BlockSpec((d, TB), lambda i: (0, part * steps + i)), DONE],
        out_shape=[jax.ShapeDtypeStruct((t, d), BF), jax.ShapeDtypeStruct((d, t), BF), jax.ShapeDtypeStruct((8, 128), F32)],
        input_output_aliases={6 + i: i for i in range(len(more))},
        compiler_params=params(),
        cost_estimate=cost(4 * t * d * ff / parts, 4 * t * ff / parts),
        name="input_gradient",
    )(dg, du, wg, wu, h, dy, *more)


def adamw(w, m, v, g):
    m = 0.9 * m + 0.1 * g
    v = 0.95 * v + 0.05 * g * g
    step = m * lax.rsqrt(v + 1e-8) + 0.1 * w
    return (w - 0.02 * step).astype(BF), m, v


def gather_block(pos_ref, side, first, refs, scr):
    rows = scr.shape[0] // side**2
    y, nxt, far_a, far_b, prv = refs
    half = side // 2
    for r0 in range(side):
        for r1 in range(side):
            if r0 == 2:
                ref, k = (far_a, r1) if r1 < half else (far_b, r1 - half)
            else:
                ref, k = {0: y, 1: nxt, 3: prv}[r0], r1
            at = lax.rem(pos_ref[first] + r0, side) * side + lax.rem(pos_ref[first + 1] + r1, side)
            scr[pl.ds(pl.multiple_of(at * rows, 8), rows), :] = ref[k, 0].astype(F32)


def adamw_kernel(side, pos_ref, f_ref, *refs):
    pieces, w, m, v = refs[:5], refs[5:8], refs[8:11], refs[11:14]
    scr, done_ref = refs[-1], refs[-2]
    out = refs[-11:-2]
    done_ref[...] = jnp.zeros_like(done_ref)
    gather_block(pos_ref, side, 1, pieces, scr)
    f = f_ref[0]
    for i in range(3):
        g = scr[:, i * FB : (i + 1) * FB]
        if i == 2:
            g = g.T
        out[i][0], out[3 + i][0], out[6 + i][0] = adamw(w[i][0].astype(F32), m[i][0], v[i][0], g * f)


def update_half(side, layer, pos, factor, pieces, w, m, v, sofar):
    d, ff = w[0].shape[1:]
    nb = ff // (2 * FB)
    wide = pl.BlockSpec((1, d, FB), lambda j, p: (layer, 0, p[0] * nb + j))
    tall = pl.BlockSpec((1, FB, d), lambda j, p: (layer, p[0] * nb + j, 0))
    three = [wide, wide, tall]
    g_specs = [pl.BlockSpec((a.shape[0], 1) + a.shape[2:], lambda j, p: (0, j, 0, 0)) for a in pieces]
    more = [] if sofar is None else list(sofar)
    return pl.pallas_call(
        functools.partial(adamw_kernel, side),
        grid_spec=pltpu.PrefetchScalarGridSpec(
            num_scalar_prefetch=1,
            grid=(nb,),
            in_specs=[pl.BlockSpec(memory_space=pltpu.SMEM)] + g_specs + three * 3 + [pl.BlockSpec(memory_space=pl.ANY)] * len(more),
            out_specs=three * 3 + [DONE],
            scratch_shapes=[pltpu.VMEM((d, 3 * FB), F32)],
        ),
        out_shape=[jax.ShapeDtypeStruct(a.shape, a.dtype) for a in (*w, *m, *v)] + [jax.ShapeDtypeStruct((8, 128), F32)],
        input_output_aliases={16 + i: i for i in range(len(more))},
        compiler_params=params(),
        cost_estimate=cost(4000 * d * ff, 33 * d * ff),
        name="adamw",
    )(pos, factor, *pieces, *w, *m, *v, *more)


def total(*terms):
    return sum(term.astype(F32) for term in terms)


def solution(mesh):
    n = mesh.shape["dp"]
    side = math.isqrt(n // 2)
    assert side == 4 and 2 * side * side == n

    def ring(stage, by):
        pairs = []
        for i in range(n):
            chip, core = divmod(i, 2)
            x, y = divmod(chip, side)
            if (core + stage) % 2 == 0:
                x = (x + by) % side
            else:
                y = (y + by) % side
            pairs.append((i, (x * side + y) * 2 + core))
        return lambda a: lax.ppermute(a, "dp", pairs)

    other_core = lambda a: lax.ppermute(a, "dp", [(i, i ^ 1) for i in range(n)])

    def chain(mine, recv):
        def sent(moves, arrays, ran):
            got = [move(a) for move, a in zip(moves, arrays, strict=True)]
            return lax.optimization_barrier((*got, *ran))[: len(got)] if ran else got

        on, back = ring(0, 1), ring(0, -1)
        q, h = side, side // 2
        chip = lambda r0, lo, hi: (mine[r0 * q + lo : r0 * q + hi], recv[r0 * q + lo : r0 * q + hi])
        send = [total(*chip(*part)).astype(BF) for part in ((2, 0, h), (2, h, q), (1, h, q), (3, 0, h))]
        ran = yield send
        far_a, far_b, n_b, p_a = sent((on, back, on, back), send, ran)
        send = [total(*chip(1, 0, h), far_a).astype(BF), total(*chip(3, h, q), far_b).astype(BF)]
        ran = yield send
        n_a, p_b = sent((on, back), send, ran)
        low, high = total(*chip(0, 0, h), n_a, p_a), total(*chip(0, h, q), n_b, p_b)
        moves = [ring(1, k) for k in range(1, q)]
        send = [low[1].astype(BF), high[0].astype(BF), high[1].astype(BF)]
        ran = yield send
        own = total(low[0], *sent(moves, send, ran)).astype(BF)
        ran = yield [own]
        y = jnp.stack([own, *sent(moves, [own] * len(moves), ran)[::-1]])
        ran = yield [y]
        prv, nxt = sent((on, back), [y, y], ran)
        send = [prv[:h], nxt[h:]]
        ran = yield send
        far_a, far_b = sent((on, back), send, ran)
        mine = (y, nxt, far_a, far_b, prv)
        ran = yield mine
        yield sent((other_core,) * len(mine), mine, ran)

    def sum_of_all(s):
        s = jnp.full((8, 128), s, F32)
        for moves in ((other_core,), [ring(0, k) for k in range(1, side)], [ring(1, k) for k in range(1, side)]):
            s = s + sum(move(s) for move in moves)
        return s[0, 0]

    def step(x, dy, *arrays):
        w, m, v = (arrays[i : i + 3] for i in (0, 3, 6))
        layers = w[0].shape[0]
        assert layers == 2
        index = lax.axis_index("dp")
        core, at_y, at_x = lax.rem(index, 2), lax.rem(index // 2, side), index // (2 * side)
        at0, at1 = jnp.where(core == 0, at_x, at_y), jnp.where(core == 0, at_y, at_x)
        own_half = jnp.stack([core, at0, at1]).astype(jnp.int32)
        other_half = jnp.stack([1 - core, at1, at0]).astype(jnp.int32)

        after = lambda a, before: lax.optimization_barrier((a, *before))[0]

        x, dy = x[0], dy[0]
        nb = w[0].shape[2] // (2 * FB)
        h1, a1, a1t, a0t, dyt, gate, up = forward(0, x, dy, *w)
        given, by_gate, by_up = last_half(side, 1, other_half, a1, a1t, dy, dyt, *w, None)
        recv = other_core(given)
        mine, by_gate, by_up = last_half(side, 1, after(own_half, [given]), a1, a1t, dy, dyt, *w, (by_gate, by_up))
        top = chain(mine, recv)
        *dh, ran = input_gradient(1, 0, 2, by_gate, by_up, w[0], w[1], after(h1, next(top)), dy, None)
        dh, dht, ran = input_gradient(1, 1, 2, by_gate, by_up, w[0], w[1], after(h1, top.send([ran])), dy, dh)
        given, ran = inner_half(side, 0, 0, nb, after(other_half, top.send([ran])), gate, up, a0t, dh, dht, w[2], None)
        recv = other_core(given)
        top_send = top.send([ran])
        top_piece = top_send[0]
        mine, ran = inner_half(side, 0, 0, nb // 2, after(own_half, [given, *top_send]), gate, up, a0t, dh, dht, w[2], None)
        mine, ran = inner_half(side, 0, nb // 2, nb, after(own_half, top.send([ran])), gate, up, a0t, dh, dht, w[2], mine)
        bottom = chain(mine, recv)
        top.send([ran])
        top_mine = next(top)
        for _ in range(4):
            bottom_piece = next(bottom)[0]
        squares = sum_of_all(sum(jnp.sum(total(p) ** 2) for p in (top_piece, bottom_piece)))
        count = sum(a.size for a in w)
        factor = jnp.minimum(1.0, 0.5 * lax.rsqrt(squares / count + 1e-30)).reshape(1)

        *new, ran = update_half(side, 1, after(own_half, [*next(bottom), *top_mine]), factor, top_mine, w, m, v, None)
        *new, ran = update_half(side, 1, after(other_half, bottom.send([ran])), factor, top.send([ran]), w, m, v, new)
        bottom_mine = bottom.send([ran])
        *new, ran = update_half(side, 0, after(own_half, bottom_mine), factor, bottom_mine, w, m, v, new)
        *new, ran = update_half(side, 0, other_half, factor, bottom.send([ran]), w, m, v, new)
        return tuple(new)

    return jax.shard_map(
        step,
        mesh=mesh,
        in_specs=(P(("rep", "dp"), None, None),) * 2 + (P(None, None, None),) * 9,
        out_specs=(P("rep", None, None),) * 9,
        check_vma=False,
    )
```

```python
import functools
import math

import jax
import jax.numpy as jnp
from jax import lax
from jax.experimental import pallas as pl
from jax.experimental.pallas import tpu as pltpu
from jax.sharding import PartitionSpec as P


BF, F32 = jnp.bfloat16, jnp.float32
FB = 256
TB = 512
VMEM = 62 * 2**20
MESH = pl.DeviceIdType.MESH
NT = (((1,), (1,)), ((), ()))
DONE = pl.BlockSpec((8, 128), lambda *_: (0, 0))


def dot(a, b):
    return jnp.dot(a, b, preferred_element_type=F32)


def dot_nt(a, b):
    return lax.dot_general(a, b, NT, preferred_element_type=F32)


def norm_scale(wide):
    return lax.rsqrt(jnp.mean(wide * wide, -1, keepdims=True) + 1e-6)


def cost(flops, moved):
    return pl.CostEstimate(flops=int(flops), bytes_accessed=int(moved), transcendentals=0)


def params(vmem=VMEM):
    return pltpu.CompilerParams(vmem_limit_bytes=vmem, dimension_semantics=("arbitrary",))


def once(shape, index):
    return pl.BlockSpec(shape, index, pipeline_mode=pl.Buffered(1))


def forward_kernel(h_ref, dy_ref, wg_ref, wu_ref, wd_ref, h1_ref, a1_ref, a1t_ref, a0t_ref, dyt_ref, gate_ref, up_ref, hid):
    ff = wg_ref.shape[2]
    h = h_ref[...]
    wide = h.astype(F32)
    a = (wide * norm_scale(wide)).astype(BF)
    a0t_ref[...] = a.T
    dyt_ref[...] = dy_ref[...].T
    for j in range(0, ff, FB):
        gate = dot(a, wg_ref[0, :, j : j + FB])
        up = dot(a, wu_ref[0, :, j : j + FB])
        gate_ref[:, j : j + FB] = gate
        up_ref[:, j : j + FB] = up
        hid[:, j : j + FB] = (gate * lax.logistic(gate) * up).astype(BF)
    out = dot(hid[...], wd_ref[0]).astype(BF)
    h1 = (h.astype(F32) + out.astype(F32)).astype(BF)
    h1_ref[...] = h1
    wide = h1.astype(F32)
    a1 = (wide * norm_scale(wide)).astype(BF)
    a1_ref[...] = a1
    a1t_ref[...] = a1.T


def forward(layer, h, dy, wg, wu, wd):
    t, d = h.shape
    ff = wg.shape[2]
    rows = pl.BlockSpec((TB, d), lambda i: (i, 0))
    cols = pl.BlockSpec((d, TB), lambda i: (0, i))
    wide = pl.BlockSpec((TB, ff), lambda i: (i, 0))
    whole = [once((1,) + w.shape[1:], lambda i: (layer, 0, 0)) for w in (wg, wu, wd)]
    act, actt = jax.ShapeDtypeStruct((t, d), BF), jax.ShapeDtypeStruct((d, t), BF)
    kept = jax.ShapeDtypeStruct((t, ff), F32)
    return pl.pallas_call(
        forward_kernel,
        grid=(t // TB,),
        in_specs=[rows, rows] + whole,
        out_specs=[rows, rows, cols, cols, cols, wide, wide],
        out_shape=[act, act, actt, actt, actt, kept, kept],
        scratch_shapes=[pltpu.VMEM((TB, ff), BF)],
        compiler_params=params(),
        cost_estimate=cost(6 * t * d * ff, 8 * t * ff),
        name="forward",
    )(h, dy, wg, wu, wd)


def spread(pos_ref, side, scr, g_ref):
    rows = scr.shape[0] // side**2
    for r0 in range(side):
        for r1 in range(side):
            at = lax.rem(pos_ref[1] + r0, side) * side + lax.rem(pos_ref[2] + r1, side)
            g_ref[r0 * side + r1, 0] = scr[pl.ds(pl.multiple_of(at * rows, 8), rows), :].astype(BF)


def backward_of_hidden(gate, up, dh):
    s = lax.logistic(gate)
    silu = gate * s
    by_silu = dh * up
    return (silu * up).astype(BF), (by_silu * (s + silu * (1.0 - s))).astype(BF), (dh * silu).astype(BF)


def weight_gradients(scr, at_ref, dyt_ref, hid, dg_ref, du_ref):
    scr[:, :FB] = dot(at_ref[...], dg_ref[...])
    scr[:, FB : 2 * FB] = dot(at_ref[...], du_ref[...])
    scr[:, 2 * FB :] = dot(dyt_ref[...], hid[...])


def last_kernel(side, pos_ref, a_ref, at_ref, dy_ref, dyt_ref, wg_ref, wu_ref, wd_ref, *rest):
    g_ref, dg_ref, du_ref, hid, scr = rest[-5:]
    for c in range(0, a_ref.shape[0], TB):
        here = slice(c, c + TB)
        gate = dot(a_ref[here, :], wg_ref[0])
        up = dot(a_ref[here, :], wu_ref[0])
        dh = dot_nt(dy_ref[here, :], wd_ref[0]).astype(BF).astype(F32)
        hid[here, :], dg_ref[here, :], du_ref[here, :] = backward_of_hidden(gate, up, dh)
    weight_gradients(scr, at_ref, dyt_ref, hid, dg_ref, du_ref)
    spread(pos_ref, side, scr, g_ref)


def inner_kernel(side, pos_ref, gate_ref, up_ref, at_ref, dy_ref, dyt_ref, wd_ref, *rest):
    g_ref, done_ref, hid, dg, du, scr = rest[-6:]
    done_ref[...] = jnp.zeros_like(done_ref)
    for c in range(0, dy_ref.shape[0], TB):
        here = slice(c, c + TB)
        dh = dot_nt(dy_ref[here, :], wd_ref[0]).astype(BF).astype(F32)
        hid[here, :], dg[here, :], du[here, :] = backward_of_hidden(gate_ref[here, :], up_ref[here, :], dh)
    weight_gradients(scr, at_ref, dyt_ref, hid, dg, du)
    spread(pos_ref, side, scr, g_ref)


def piece_shape(side, d, ff):
    return (side**2, ff // (2 * FB), d // side**2, 3 * FB)


def last_half(side, layer, pos, a, at, dy, dyt, wg, wu, wd, sofar):
    t, d = a.shape
    ff = wg.shape[2]
    nb = ff // (2 * FB)
    whole = [once((t, d), lambda j, p: (0, 0)), once((d, t), lambda j, p: (0, 0))] * 2
    up_block = pl.BlockSpec((1, d, FB), lambda j, p: (layer, 0, p[0] * nb + j))
    down_block = pl.BlockSpec((1, FB, d), lambda j, p: (layer, p[0] * nb + j, 0))
    by_gate = pl.BlockSpec((t, FB), lambda j, p: (0, p[0] * nb + j))
    shape = piece_shape(side, d, ff)
    g_block = pl.BlockSpec((shape[0], 1) + shape[2:], lambda j, p: (0, j, 0, 0))
    kept = jax.ShapeDtypeStruct((t, ff), BF)
    more = [] if sofar is None else list(sofar)
    return pl.pallas_call(
        functools.partial(last_kernel, side),
        grid_spec=pltpu.PrefetchScalarGridSpec(
            num_scalar_prefetch=1,
            grid=(nb,),
            in_specs=whole + [up_block, up_block, down_block] + [pl.BlockSpec(memory_space=pl.ANY)] * len(more),
            out_specs=[g_block, by_gate, by_gate],
            scratch_shapes=[pltpu.VMEM((t, FB), BF), pltpu.VMEM((d, 3 * FB), F32)],
        ),
        out_shape=[jax.ShapeDtypeStruct(shape, BF), kept, kept],
        input_output_aliases={8 + i: 1 + i for i in range(len(more))},
        compiler_params=params(),
        cost_estimate=cost(6 * t * d * ff, 2 * t * ff),
        name="last_half",
    )(pos, a, at, dy, dyt, wg, wu, wd, *more)


def inner_half(side, layer, first, last, pos, gate, up, at, dy, dyt, wd, sofar):
    t, d = dy.shape
    ff = wd.shape[1]
    nb = ff // (2 * FB)
    kept = pl.BlockSpec((t, FB), lambda j, p: (0, p[0] * nb + first + j))
    rows, cols = once((t, d), lambda j, p: (0, 0)), once((d, t), lambda j, p: (0, 0))
    down_block = pl.BlockSpec((1, FB, d), lambda j, p: (layer, p[0] * nb + first + j, 0))
    shape = piece_shape(side, d, ff)
    more = [] if sofar is None else [sofar]
    share = (last - first) / nb
    return pl.pallas_call(
        functools.partial(inner_kernel, side),
        grid_spec=pltpu.PrefetchScalarGridSpec(
            num_scalar_prefetch=1,
            grid=(last - first,),
            in_specs=[kept, kept, cols, rows, cols, down_block] + [pl.BlockSpec(memory_space=pl.ANY)] * len(more),
            out_specs=[pl.BlockSpec((shape[0], 1) + shape[2:], lambda j, p: (0, first + j, 0, 0)), DONE],
            scratch_shapes=[pltpu.VMEM((t, FB), BF)] * 3 + [pltpu.VMEM((d, 3 * FB), F32)],
        ),
        out_shape=[jax.ShapeDtypeStruct(shape, BF), jax.ShapeDtypeStruct((8, 128), F32)],
        input_output_aliases={7 + i: i for i in range(len(more))},
        compiler_params=params(),
        cost_estimate=cost(4 * t * d * ff * share, 4 * t * ff * share),
        name="inner_half",
    )(pos, gate, up, at, dy, dyt, wd, *more)


def input_kernel(dg_ref, du_ref, wg_ref, wu_ref, h_ref, dy_ref, *rest):
    dh_ref, dht_ref, done_ref = rest[-3:]
    done_ref[...] = jnp.zeros_like(done_ref)
    da = dot_nt(dg_ref[...], wg_ref[0]).astype(BF).astype(F32) + dot_nt(du_ref[...], wu_ref[0]).astype(BF).astype(F32)
    da = da.astype(BF).astype(F32)
    wide = h_ref[...].astype(F32)
    s = norm_scale(wide)
    by_wide = da * s - wide * (s * s * s * jnp.mean(da * wide, -1, keepdims=True))
    dh = (dy_ref[...].astype(F32) + by_wide.astype(BF).astype(F32)).astype(BF)
    dh_ref[...] = dh
    dht_ref[...] = dh.T


def input_gradient(layer, part, parts, dg, du, wg, wu, h, dy, sofar):
    t, d = h.shape
    ff = wg.shape[2]
    steps = t // TB // parts
    rows = pl.BlockSpec((TB, d), lambda i: (part * steps + i, 0))
    wide = pl.BlockSpec((TB, ff), lambda i: (part * steps + i, 0))
    whole = once((1, d, ff), lambda i: (layer, 0, 0))
    more = [] if sofar is None else list(sofar)
    return pl.pallas_call(
        input_kernel,
        grid=(steps,),
        in_specs=[wide, wide, whole, whole, rows, rows] + [pl.BlockSpec(memory_space=pl.ANY)] * len(more),
        out_specs=[rows, pl.BlockSpec((d, TB), lambda i: (0, part * steps + i)), DONE],
        out_shape=[jax.ShapeDtypeStruct((t, d), BF), jax.ShapeDtypeStruct((d, t), BF), jax.ShapeDtypeStruct((8, 128), F32)],
        input_output_aliases={6 + i: i for i in range(len(more))},
        compiler_params=params(),
        cost_estimate=cost(4 * t * d * ff / parts, 4 * t * ff / parts),
        name="input_gradient",
    )(dg, du, wg, wu, h, dy, *more)


def adamw(w, m, v, g):
    m = 0.9 * m + 0.1 * g
    v = 0.95 * v + 0.05 * g * g
    step = m * lax.rsqrt(v + 1e-8) + 0.1 * w
    return (w - 0.02 * step).astype(BF), m, v


def gather_block(pos_ref, side, first, refs, scr):
    rows = scr.shape[0] // side**2
    y, nxt, far_a, far_b, prv = refs
    half = side // 2
    for r0 in range(side):
        for r1 in range(side):
            if r0 == 2:
                ref, k = (far_a, r1) if r1 < half else (far_b, r1 - half)
            else:
                ref, k = {0: y, 1: nxt, 3: prv}[r0], r1
            at = lax.rem(pos_ref[first] + r0, side) * side + lax.rem(pos_ref[first + 1] + r1, side)
            scr[pl.ds(pl.multiple_of(at * rows, 8), rows), :] = ref[k, 0].astype(F32)


def adamw_kernel(side, pos_ref, f_ref, *refs):
    pieces, w, m, v = refs[:5], refs[5:8], refs[8:11], refs[11:14]
    scr, done_ref = refs[-1], refs[-2]
    out = refs[-11:-2]
    done_ref[...] = jnp.zeros_like(done_ref)
    gather_block(pos_ref, side, 1, pieces, scr)
    f = f_ref[0]
    for i in range(3):
        g = scr[:, i * FB : (i + 1) * FB]
        if i == 2:
            g = g.T
        out[i][0], out[3 + i][0], out[6 + i][0] = adamw(w[i][0].astype(F32), m[i][0], v[i][0], g * f)


def update_half(side, layer, pos, factor, pieces, w, m, v, sofar):
    d, ff = w[0].shape[1:]
    nb = ff // (2 * FB)
    wide = pl.BlockSpec((1, d, FB), lambda j, p: (layer, 0, p[0] * nb + j))
    tall = pl.BlockSpec((1, FB, d), lambda j, p: (layer, p[0] * nb + j, 0))
    three = [wide, wide, tall]
    g_specs = [pl.BlockSpec((a.shape[0], 1) + a.shape[2:], lambda j, p: (0, j, 0, 0)) for a in pieces]
    more = [] if sofar is None else list(sofar)
    return pl.pallas_call(
        functools.partial(adamw_kernel, side),
        grid_spec=pltpu.PrefetchScalarGridSpec(
            num_scalar_prefetch=1,
            grid=(nb,),
            in_specs=[pl.BlockSpec(memory_space=pltpu.SMEM)] + g_specs + three * 3 + [pl.BlockSpec(memory_space=pl.ANY)] * len(more),
            out_specs=three * 3 + [DONE],
            scratch_shapes=[pltpu.VMEM((d, 3 * FB), F32)],
        ),
        out_shape=[jax.ShapeDtypeStruct(a.shape, a.dtype) for a in (*w, *m, *v)] + [jax.ShapeDtypeStruct((8, 128), F32)],
        input_output_aliases={16 + i: i for i in range(len(more))},
        compiler_params=params(),
        cost_estimate=cost(4000 * d * ff, 33 * d * ff),
        name="adamw",
    )(pos, factor, *pieces, *w, *m, *v, *more)


def total(*terms):
    return sum(term.astype(F32) for term in terms)


def device(side, x, y, core):
    return {"dp": (lax.rem(x, side) * side + lax.rem(y, side)) * 2 + core}


def place(side):
    me = lax.axis_index("dp")
    return me // (2 * side), lax.rem(me // 2, side), lax.rem(me, 2)


def along(side, stage, by):
    x, y, core = place(side)
    on_y = lax.rem(core + stage, 2)
    return device(side, x + by * (1 - on_y), y + by * on_y, core)


def meet(devices):
    barrier = pltpu.get_barrier_semaphore()
    for one in devices:
        pl.semaphore_signal(barrier, inc=1, device_id=one, device_id_type=MESH)
    pl.semaphore_wait(barrier, len(devices))


def each_block(count, nb, do):
    def outer(k, _):
        def inner(j, _):
            do(k, j)
            return 0

        return lax.fori_loop(0, nb, inner, 0)

    lax.fori_loop(0, count, outer, 0)


def first_ring_kernel(side, mine, recv, out, send, got, send_sem, got_sem):
    nb, h = mine.shape[1], side // 2
    peers = along(side, 0, 1), along(side, 0, side - 1)
    meet(peers)

    def fill(slot, first, *more):
        def do(k, j):
            terms = [mine[first + k, j], recv[first + k, j]] + [got[at, k, j] for at in more]
            send[slot, k, j] = total(*terms).astype(BF)

        each_block(h, nb, do)

    def copy(slot):
        return pltpu.make_async_remote_copy(
            src_ref=send.at[slot],
            dst_ref=got.at[slot],
            send_sem=send_sem.at[slot],
            recv_sem=got_sem.at[slot],
            device_id=peers[slot % 2],
            device_id_type=MESH,
        )

    for slot, first in enumerate((2 * side, 2 * side + h, side + h, 3 * side)):
        fill(slot, first)
        copy(slot).start()
    for slot, first in ((4, side), (5, 3 * side + h)):
        copy(slot - 4).wait_recv()
        fill(slot, first, slot - 4)
        copy(slot).start()
    for slot in (2, 3, 4, 5):
        copy(slot).wait_recv()
    for first, one, two in ((0, 4, 3), (h, 2, 5)):

        def do(k, j, first=first, one=one, two=two):
            out[first + k, j] = total(mine[first + k, j], recv[first + k, j], got[one, k, j], got[two, k, j])

        each_block(h, nb, do)
    for slot in range(6):
        copy(slot).wait_send()


def first_ring(side, mine, recv):
    shape = (side // 2,) + mine.shape[1:]
    return pl.pallas_call(
        functools.partial(first_ring_kernel, side),
        in_specs=[pl.BlockSpec(memory_space=pltpu.VMEM)] * 2,
        out_specs=pl.BlockSpec(memory_space=pltpu.VMEM),
        out_shape=jax.ShapeDtypeStruct((side,) + mine.shape[1:], F32),
        scratch_shapes=[pltpu.VMEM((6,) + shape, BF), pltpu.VMEM((6,) + shape, BF), pltpu.SemaphoreType.DMA((6,)), pltpu.SemaphoreType.DMA((6,))],
        compiler_params=pltpu.CompilerParams(vmem_limit_bytes=VMEM, collective_id=24, has_side_effects=True),
        cost_estimate=cost(3e10, 3e7),
        name="first_ring",
    )(mine, recv)


def second_ring_kernel(side, own, squares, y, all_squares, send, got, sums, sem, y_sem, sum_sem):
    nb = own.shape[1]
    steps = range(1, side)
    at_x, at_y, core = place(side)
    by_x = [device(side, at_x + k, at_y, core) for k in steps]
    by_y = [device(side, at_x, at_y + k, core) for k in steps]
    partner = device(side, at_x, at_y, 1 - core)
    meet([partner, *by_x, *by_y])

    def move(src, dst, sems, at, to):
        return pltpu.make_async_remote_copy(src_ref=src, dst_ref=dst, send_sem=sems.at[0, at], recv_sem=sems.at[1, at], device_id=to, device_id_type=MESH)

    pieces = [move(send.at[k - 1], got.at[k - 1], sem, k - 1, along(side, 1, k)) for k in steps]
    for k in (2, 1, 3):

        def do(_, j, k=k):
            send[k - 1, j] = own[k, j].astype(BF)

        each_block(1, nb, do)
        pieces[k - 1].start()
    for one in pieces:
        one.wait_recv()
    sums[0] = squares[...]

    def do(_, j):
        piece = total(own[0, j], *[got[k - 1, j] for k in steps]).astype(BF)
        y[0, j] = piece
        square = jnp.square(piece.astype(F32))
        folded = sum(square[r : r + 8, c : c + 128] for r in range(0, square.shape[0], 8) for c in range(0, square.shape[1], 128))
        sums[0] += folded

    each_block(1, nb, do)
    shards = [move(y.at[0], y.at[side - k], y_sem, k - 1, along(side, 1, k)) for k in steps]
    for k in (2, 1, 3):
        shards[k - 1].start()
    across = move(sums.at[0], sums.at[1], sum_sem, 0, partner)
    across.start()
    across.wait_recv()
    together = sums[0] + sums[1]
    waits = [across]
    for slots, at, first, peers in ((2, at_x, 1, by_x), (2 + side, at_y, side, by_y)):
        sums[slots + at] = together
        copies = [move(sums.at[slots + at], sums.at[slots + at], sum_sem, first + k - 1, peers[k - 1]) for k in steps]
        for one in copies:
            one.start()
        for one in copies:
            one.wait_recv()
        together = sums[slots]
        for i in steps:
            together += sums[slots + i]
        waits += copies
    all_squares[...] = together
    for one in shards:
        one.wait_recv()
    for one in (*pieces, *shards, *waits):
        one.wait_send()


def second_ring(side, own, squares):
    piece = own.shape[1:]
    vmem = pl.BlockSpec(memory_space=pltpu.VMEM)
    dma = pltpu.SemaphoreType.DMA
    return pl.pallas_call(
        functools.partial(second_ring_kernel, side),
        in_specs=[vmem] * 2,
        out_specs=[vmem] * 2,
        out_shape=[jax.ShapeDtypeStruct(own.shape, BF), jax.ShapeDtypeStruct(squares.shape, F32)],
        scratch_shapes=[
            pltpu.VMEM((side - 1,) + piece, BF),
            pltpu.VMEM((side - 1,) + piece, BF),
            pltpu.VMEM((2 + 2 * side,) + squares.shape, F32),
            dma((2, side - 1)),
            dma((2, side - 1)),
            dma((2, 2 * side - 1)),
        ],
        compiler_params=pltpu.CompilerParams(vmem_limit_bytes=VMEM, collective_id=25, has_side_effects=True),
        cost_estimate=cost(3e10, 1e7),
        name="second_ring",
    )(own, squares)


def solution(mesh):
    n = mesh.shape["dp"]
    side = math.isqrt(n // 2)
    assert side == 4 and 2 * side * side == n

    def ring(stage, by):
        pairs = []
        for i in range(n):
            chip, core = divmod(i, 2)
            x, y = divmod(chip, side)
            if (core + stage) % 2 == 0:
                x = (x + by) % side
            else:
                y = (y + by) % side
            pairs.append((i, (x * side + y) * 2 + core))
        return lambda a: lax.ppermute(a, "dp", pairs)

    other_core = lambda a: lax.ppermute(a, "dp", [(i, i ^ 1) for i in range(n)])

    def sent(moves, arrays, ran):
        got = [move(a) for move, a in zip(moves, arrays, strict=True)]
        return lax.optimization_barrier((*got, *ran))[: len(got)] if ran else got

    def chain(mine, recv):
        on, back = ring(0, 1), ring(0, -1)
        q, h = side, side // 2
        chip = lambda r0, lo, hi: (mine[r0 * q + lo : r0 * q + hi], recv[r0 * q + lo : r0 * q + hi])
        send = [total(*chip(*part)).astype(BF) for part in ((2, 0, h), (2, h, q), (1, h, q), (3, 0, h))]
        ran = yield send
        far_a, far_b, n_b, p_a = sent((on, back, on, back), send, ran)
        send = [total(*chip(1, 0, h), far_a).astype(BF), total(*chip(3, h, q), far_b).astype(BF)]
        ran = yield send
        n_a, p_b = sent((on, back), send, ran)
        low, high = total(*chip(0, 0, h), n_a, p_a), total(*chip(0, h, q), n_b, p_b)
        moves = [ring(1, k) for k in range(1, q)]
        send = [low[1].astype(BF), high[0].astype(BF), high[1].astype(BF)]
        ran = yield send
        own = total(low[0], *sent(moves, send, ran)).astype(BF)
        ran = yield [own]
        y = jnp.stack([own, *sent(moves, [own] * len(moves), ran)[::-1]])
        yield from rest_of_gather(y)

    def rest_of_gather(y):
        on, back = ring(0, 1), ring(0, -1)
        h = side // 2
        ran = yield [y]
        prv, nxt = sent((on, back), [y, y], ran)
        send = [prv[:h], nxt[h:]]
        ran = yield send
        far_a, far_b = sent((on, back), send, ran)
        mine = (y, nxt, far_a, far_b, prv)
        ran = yield mine
        yield sent((other_core,) * len(mine), mine, ran)

    def step(x, dy, *arrays):
        w, m, v = (arrays[i : i + 3] for i in (0, 3, 6))
        layers = w[0].shape[0]
        assert layers == 2
        index = lax.axis_index("dp")
        core, at_y, at_x = lax.rem(index, 2), lax.rem(index // 2, side), index // (2 * side)
        at0, at1 = jnp.where(core == 0, at_x, at_y), jnp.where(core == 0, at_y, at_x)
        own_half = jnp.stack([core, at0, at1]).astype(jnp.int32)
        other_half = jnp.stack([1 - core, at1, at0]).astype(jnp.int32)

        return whole(x[0], dy[0], w, m, v, own_half, other_half)

    after = lambda a, before: lax.optimization_barrier((a, *before))[0]

    def whole(x, dy, w, m, v, own_half, other_half):
        nb = w[0].shape[2] // (2 * FB)
        h1, a1, a1t, a0t, dyt, gate, up = forward(0, x, dy, *w)
        given, by_gate, by_up = last_half(side, 1, other_half, a1, a1t, dy, dyt, *w, None)
        recv = other_core(given)
        mine, by_gate, by_up = last_half(side, 1, after(own_half, [given]), a1, a1t, dy, dyt, *w, (by_gate, by_up))
        top = chain(mine, recv)
        *dh, ran = input_gradient(1, 0, 2, by_gate, by_up, w[0], w[1], after(h1, next(top)), dy, None)
        dh, dht, ran = input_gradient(1, 1, 2, by_gate, by_up, w[0], w[1], after(h1, top.send([ran])), dy, dh)
        before = after(other_half, top.send([ran]))
        given, ran = inner_half(side, 0, 0, nb, before, gate, up, a0t, dh, dht, w[2], None)
        recv = other_core(given)
        top_send = top.send([ran])
        top_piece = top_send[0]
        before = after(own_half, [given, *top_send])
        mine, ran = inner_half(side, 0, 0, nb // 2, before, gate, up, a0t, dh, dht, w[2], None)
        mine, ran = inner_half(side, 0, nb // 2, nb, after(own_half, top.send([ran])), gate, up, a0t, dh, dht, w[2], mine)
        squares = jnp.full((8, 128), jnp.sum(total(top_piece) ** 2) / (8 * 128))
        own = first_ring(side, mine, recv)
        y, squares = second_ring(side, own, after(squares, top.send([ran])))
        bottom = rest_of_gather(y)
        top_mine = top.send([squares])
        count = sum(a.size for a in w)
        factor = jnp.minimum(1.0, 0.5 * lax.rsqrt(jnp.sum(squares) / count + 1e-30)).reshape(1)

        *new, ran = update_half(side, 1, after(own_half, [*next(bottom), *top_mine]), factor, top_mine, w, m, v, None)
        *new, ran = update_half(side, 1, after(other_half, bottom.send([ran])), factor, top.send([ran]), w, m, v, new)
        bottom_mine = bottom.send([ran])
        *new, ran = update_half(side, 0, after(own_half, bottom_mine), factor, bottom_mine, w, m, v, new)
        *new, ran = update_half(side, 0, other_half, factor, bottom.send([ran]), w, m, v, new)
        return tuple(new)

    return jax.shard_map(
        step,
        mesh=mesh,
        in_specs=(P(("rep", "dp"), None, None),) * 2 + (P(None, None, None),) * 9,
        out_specs=(P("rep", None, None),) * 9,
        check_vma=False,
    )
```
